64 devices in a mesh: dp: 4 (over x, y), stage: 16 (over z, core).
Axes of the slice: x: 2, y: 2, z: 8, core: 2. Of those that a mesh axis runs over, the one named last changes fastest.
The devices are a block of a 4x4x8 slice.
Arguments:
- inputs: bfloat16 [256, 1024, 128], P('dp'), parts along dimension 0
- targets: bfloat16 [256, 1024, 128], P('dp'), parts along dimension 0
- w_up: bfloat16 [16, 128, 512], P('stage')
- w_down: bfloat16 [16, 512, 128], P('stage')
- gains: float32 [16, 128], P('stage')
Outputs:
- output 1: float32 [4], P('dp'), parts along dimension 0
- output 2: float32 [64, 128, 512], P(('dp', 'stage')), parts along dimension 0
- output 3: float32 [64, 512, 128], P(('dp', 'stage')), parts along dimension 0
- output 4: float32 [64, 128], P(('dp', 'stage')), parts along dimension 0
There are 4 independent parts. The reference program is written for one: setup_inputs(seed, part) draws one part's arguments, and reference() takes and returns one part's arrays. A program takes and returns all parts, laid end to end along the dimension named above; an argument that names none is the same for every part.
All inputs are finite; a program needn't handle non-finite values.
Results may differ from the reference program's by a relative error of at most 0.00117831.
Values are sent between devices in bfloat16 or wider.
A program may use at most 768 MiB of HBM per device.

```python
import jax
import jax.numpy as jnp
from jax import lax

NUM_MICRO = 64
MICRO_TOKENS = 1024
MODEL_DIM = 128
HIDDEN_DIM = 512
NUM_LAYERS = 16
NORM_EPS = 1e-6


def setup_inputs(seed: int = 0, part: int = 0) -> dict:
    keys = jax.random.split(jax.random.key(seed), 4)
    part_keys = jax.random.split(jax.random.fold_in(keys[0], part), 2)
    act_shape = (NUM_MICRO, MICRO_TOKENS, MODEL_DIM)
    inputs = jax.random.normal(part_keys[0], act_shape, jnp.float32)
    targets = jax.random.normal(part_keys[1], act_shape, jnp.float32)
    up_scale = MODEL_DIM ** -0.5
    down_scale = 1.5 * (HIDDEN_DIM * NUM_LAYERS) ** -0.5
    w_up = jax.random.normal(keys[1], (NUM_LAYERS, MODEL_DIM, HIDDEN_DIM), jnp.float32) * up_scale
    w_down = jax.random.normal(keys[2], (NUM_LAYERS, HIDDEN_DIM, MODEL_DIM), jnp.float32) * down_scale
    gains = 1.0 + 0.3 * jax.random.normal(keys[3], (NUM_LAYERS, MODEL_DIM), jnp.float32)
    return {'inputs': inputs.astype(jnp.bfloat16), 'targets': targets.astype(jnp.bfloat16), 'w_up': w_up.astype(jnp.bfloat16), 'w_down': w_down.astype(jnp.bfloat16), 'gains': gains}


def rms_norm(x_wide, gain):
    mean_sq = jnp.mean(x_wide * x_wide, axis=-1, keepdims=True)
    return x_wide * lax.rsqrt(mean_sq + NORM_EPS) * gain


def layer_apply(act_in, layer_params):
    gain, w_up32, w_down32 = layer_params
    x_wide = act_in.astype(jnp.float32)
    normed = rms_norm(x_wide, gain).astype(jnp.bfloat16)
    pre_act = jnp.dot(normed, w_up32.astype(jnp.bfloat16), preferred_element_type=jnp.float32)
    hidden = jax.nn.gelu(pre_act, approximate=True).astype(jnp.bfloat16)
    out_add = jnp.dot(hidden, w_down32.astype(jnp.bfloat16), preferred_element_type=jnp.float32)
    return (x_wide + out_add).astype(jnp.bfloat16)


def micro_loss(params, x_micro, y_micro):
    checkpointed = jax.checkpoint(layer_apply)

    def body(carry, layer_params):
        return checkpointed(carry, layer_params), None

    final, _ = lax.scan(body, x_micro, params)
    error_val = final.astype(jnp.float32) - y_micro.astype(jnp.float32)
    return jnp.sum(error_val * error_val) / (NUM_MICRO * MICRO_TOKENS * MODEL_DIM)


def reference(inputs, targets, w_up, w_down, gains):
    params = (gains, w_up.astype(jnp.float32), w_down.astype(jnp.float32))
    grad_fn = jax.value_and_grad(micro_loss)

    def step(carry, pair):
        loss_acc, grad_acc = carry
        value, grads = grad_fn(params, pair[0], pair[1])
        grad_acc = jax.tree.map(lambda acc_val, new_val: acc_val + new_val, grad_acc, grads)
        return (loss_acc + value, grad_acc), None

    start_val = (jnp.zeros((), jnp.float32), jax.tree.map(jnp.zeros_like, params))
    (loss_total, grad_total), _ = lax.scan(step, start_val, (inputs, targets))
    return loss_total.reshape(1), grad_total[1], grad_total[2], grad_total[0]
```

```python
import functools
import math
import jax
import jax.numpy as jnp
from jax import lax
from jax.experimental import pallas as pl
from jax.experimental.pallas import tpu as pltpu
from jax.sharding import PartitionSpec as P

NORM_EPS = 1e-6
GELU_C = math.sqrt(2.0 / math.pi)
K0 = 2.0 * GELU_C
K1 = 8.0 * GELU_C * 0.044715
TILE = 512
CHUNKS = 4
RIGHT, LEFT, PARTNER = 0, 1, 2
F32 = jnp.float32
BF16 = jnp.bfloat16
MESH = pl.DeviceIdType.MESH


def mm(a, b):
    return lax.dot_general(a, b, (((1,), (0,)), ((), ())), preferred_element_type=F32)


def mm_nt(a, b):
    return lax.dot_general(a, b, (((1,), (1,)), ((), ())), preferred_element_type=F32)


def mm_tn(a, b):
    return lax.dot_general(a, b, (((0,), (0,)), ((), ())), preferred_element_type=F32)


def inv_norm(x):
    return lax.rsqrt(jnp.sum(x * x, axis=-1, keepdims=True) + NORM_EPS * x.shape[-1])


def fold8(z):
    return jnp.sum(z.reshape(-1, 8, z.shape[-1]), axis=0)


def gelu(y):
    t = jnp.tanh(y * (K1 * (y * y) + K0))
    return (y * (1.0 + t)).astype(BF16)


def gelu_pair(y, gh):
    q = y * y
    t = jnp.tanh(y * (K1 * q + K0))
    a = 1.0 + t
    hid = y * a
    slope = a + hid * ((1.0 - t) * ((3.0 * K1) * q + K0))
    return hid.astype(BF16), (gh * slope).astype(BF16)


def kernel(n, norm_count, x_hbm, y_hbm, w_own, g_own, loss_ref, up_ref, down_ref, gain_ref,
           acts, nrm, d_buf, y_buf, q_buf, h_buf, p_buf, w_half, w_all, g_all, grads, p_recv, c_recv, r_recv, l_send, l_recv,
           in_sem, w_send, w_rsem, g_send, g_rsem, p_ssem, p_rsem, c_ssem, c_rsem, r_rsem, l_ssem, l_rsem, credit):
    n_layers, _, width, hid_dim = w_all.shape
    rows = d_buf.shape[0]
    nz = n // 2
    root = math.sqrt(width)
    nt = rows // TILE
    last = n_layers - 1
    n_all = n_layers * nt
    step_rows = width // CHUNKS
    spans = [(q * step_rows, step_rows + (8 if q == CHUNKS - 1 else 0)) for q in range(CHUNKS)]

    me = lax.axis_index('stage')
    core, chip = lax.rem(me, 2), lax.div(me, 2)
    peers = (lax.rem(me + 2, n), lax.rem(me + n - 2, n), me + 1 - 2 * core)
    flips = [me + d * (1 - 2 * lax.rem(lax.div(me, d), 2)) for d in (1 << k for k in range(n.bit_length() - 1))]

    def push(src, dst, ssem, rsem, to):
        return pltpu.make_async_remote_copy(src_ref=src, dst_ref=dst, send_sem=ssem, recv_sem=rsem, device_id={'stage': to}, device_id_type=MESH)

    def tile(i):
        return pl.ds(pl.multiple_of(i * TILE, TILE), TILE)

    barrier = pltpu.get_barrier_semaphore()
    near = list(peers) + flips[2:]
    for to in near:
        pl.semaphore_signal(barrier, inc=1, device_id={'stage': to}, device_id_type=MESH)

    own = [pltpu.make_async_copy(w_own.at[0], w_all.at[me], in_sem.at[0]), pltpu.make_async_copy(g_own.at[0], g_all.at[me], in_sem.at[1])]
    share = pl.ds(pl.multiple_of(me * rows, rows), rows)
    data = [pltpu.make_async_copy(x_hbm.at[share], acts.at[0], in_sem.at[2]), pltpu.make_async_copy(y_hbm.at[share], d_buf, in_sem.at[3])]
    for cp in own + data:
        cp.start()
    pl.semaphore_wait(barrier, len(near))
    for cp in own:
        cp.wait()

    def w_copy(layer, half, way):
        return push(w_all.at[layer, half], w_all.at[layer, half], w_send.at[way, layer, half], w_rsem.at[layer, half], peers[way])

    def g_copy(layer, way):
        return push(g_all.at[layer], g_all.at[layer], g_send.at[way, layer], g_rsem.at[layer], peers[way])

    sent = []

    def start(cp):
        cp.start()
        sent.append(cp)

    for way in (RIGHT, LEFT, PARTNER):
        start(g_copy(me, way))
    for half in (0, 1):
        for way in (RIGHT, LEFT, PARTNER):
            start(w_copy(me, half, way))

    def zero(l, c):
        grads[l] = jnp.zeros(grads.shape[1:], F32)
        return c
    lax.fori_loop(0, n_layers, zero, 0)

    reach = nz // 2
    for j in range(1, reach + 1):
        for way, layer in ((RIGHT, lax.rem(me + n - 2 * j, n)), (LEFT, lax.rem(me + 2 * j, n))):
            if j < reach or way == RIGHT:
                g_copy(layer, way).wait_recv()
                if j < reach - (way == LEFT):
                    start(g_copy(layer, way))
                start(g_copy(layer, PARTNER))
        for half in (0, 1):
            for way, layer in ((RIGHT, lax.rem(me + n - 2 * j, n)), (LEFT, lax.rem(me + 2 * j, n))):
                far = reach if way == half else reach - 1
                if j <= far:
                    w_copy(layer, half, way).wait_recv()
                    if j < far:
                        start(w_copy(layer, half, way))
                    start(w_copy(layer, half, PARTNER))

    def need(l):
        @pl.when(lax.rem(l, 2) != core)
        def _():
            g_copy(l, PARTNER).wait_recv()
            for half in (0, 1):
                w_copy(l, half, PARTNER).wait_recv()

    for cp in data:
        cp.wait()

    def norm_at(l, i):
        x = acts[l, tile(i), :].astype(F32)
        return (x * inv_norm(x) * (g_all[l][0:1, :] * (0.5 * root))).astype(BF16)

    need(0)
    for i in range(3):
        nrm[0, tile(i), :] = norm_at(0, i)
    h_buf[...] = gelu(mm(nrm[0, tile(0), :], w_all[0, 0]))
    y_buf[...] = mm(nrm[0, tile(1), :], w_all[0, 0])

    def fwd_tile(l, i):
        idx = l * nt + i
        up = jnp.minimum(idx + 2, n_all - 1)
        nx = jnp.minimum(idx + 3, n_all - 1)
        l_up, i_up = lax.div(up, nt), lax.rem(up, nt)
        l_nx, i_nx = lax.div(nx, nt), lax.rem(nx, nt)
        y = y_buf[...]
        h = h_buf[...]
        n_new = norm_at(l_nx, i_nx)
        out = acts[l, tile(i), :].astype(F32) + mm_nt(h, w_all[l, 1])
        y_new = mm(nrm[l_up, tile(i_up), :], w_all[l_up, 0])
        h_new = gelu(y)
        h_buf[...] = h_new
        y_buf[...] = y_new
        nrm[l_nx, tile(i_nx), :] = n_new
        return out.astype(BF16)

    def fwd_layer(l, c):
        need(l + 1)

        def body(i, c):
            acts[l + 1, tile(i), :] = fwd_tile(l, i)
            return c
        return lax.fori_loop(0, nt, body, c)
    lax.fori_loop(0, last, fwd_layer, 0)

    def last_tile(i, acc):
        err = fwd_tile(last, i).astype(F32) - d_buf[tile(i), :].astype(F32)
        d_buf[tile(i), :] = (err * (2.0 / norm_count)).astype(BF16)
        return acc + fold8(err * err)
    l_send[0] = lax.fori_loop(0, nt, last_tile, jnp.zeros((8, width), F32))

    def part(ref, span):
        return ref.at[pl.ds(span[0], span[1])]

    def p_copy(l, half, q):
        s = lax.div(l, 2)
        return push(part(grads.at[l, half], spans[q]), part(p_recv.at[lax.rem(s, 2), half], spans[q]), p_ssem.at[s, half, q], p_rsem.at[s, half, q], peers[PARTNER])

    def c_copy(l, half, q, way):
        s = lax.div(l, 2)
        return push(part(grads.at[l, half], spans[q]), part(c_recv.at[s, half], spans[q]), c_ssem.at[s, half, q], c_rsem.at[s, half, q], peers[way])

    def r_copy(l, half, q):
        s = lax.div(l, 2)
        return push(part(grads.at[l, half], spans[q]), part(r_recv.at[half], spans[q]), c_ssem.at[s, half, q], r_rsem.at[half, q], peers[LEFT])

    def add(l, half, q, src):
        a, m = spans[q]
        grads[l, half, pl.ds(a, m), :] += src[pl.ds(a, m), :]

    def to_root(l):
        return lax.rem(lax.div(l, 2) - chip + nz, nz)

    def duties(t):
        l0 = last - t

        @pl.when((l0 >= 0) & (lax.rem(l0 + n, 2) != core))
        def _():
            @pl.when(l0 <= last - 4)
            def _():
                pl.semaphore_wait(credit, 1)
            for half in (0, 1):
                for q in range(CHUNKS):
                    p_copy(l0, half, q).start()

        for s in range(reach + 1, 0, -1):
            l = l0 + s

            @pl.when((l >= 0) & (l <= last) & (lax.rem(l + n, 2) == core))
            def _(s=s, l=l):
                rd = to_root(l)
                slot = lax.div(l, 2)
                if s == 1:
                    for half in (0, 1):
                        for q in range(CHUNKS):
                            p_copy(l, half, q).wait_recv()
                            add(l, half, q, p_recv.at[lax.rem(slot, 2), half])

                    @pl.when(l >= 4)
                    def _():
                        pl.semaphore_signal(credit, inc=1, device_id={'stage': peers[PARTNER]}, device_id_type=MESH)
                for half in (0, 1):
                    arc_r = reach - half
                    arc_l = nz - 1 - arc_r
                    pos = s - 1
                    for way, arc, dist in ((RIGHT, arc_r, rd), (LEFT, arc_l, nz - rd)):
                        if pos < arc:
                            @pl.when(dist == arc - pos)
                            def _(half=half, way=way, arc=arc, pos=pos):
                                for q in range(CHUNKS):
                                    if pos > 0:
                                        c_copy(l, half, q, way).wait_recv()
                                        add(l, half, q, c_recv.at[slot, half])
                                    if way == LEFT and pos == arc - 1:
                                        r_copy(l, half, q).start()
                                    else:
                                        c_copy(l, half, q, way).start()
                if s == reach + 1:
                    @pl.when(rd == 0)
                    def _():
                        for half in (0, 1):
                            for q in range(CHUNKS):
                                c_copy(l, half, q, RIGHT).wait_recv()
                                add(l, half, q, c_recv.at[slot, half])
                                r_copy(l, half, q).wait_recv()
                                add(l, half, q, r_recv.at[half])

    def l_copy(k):
        return push(l_send.at[k], l_recv.at[k], l_ssem.at[k], l_rsem.at[k], flips[k])

    def loss_duties(t):
        for k in range(len(flips)):
            @pl.when(t == 2 * k)
            def _(k=k):
                l_copy(k).start()

            @pl.when(t == 2 * k + 1)
            def _(k=k):
                l_copy(k).wait()
                l_send[k + 1] = l_send[k] + l_recv[k]

    def halve(l):
        w_half[lax.rem(l, 2)] = w_all[l, 1] * jnp.asarray(0.5, BF16)

    def pre_pair(l, i):
        return mm(nrm[l, tile(i), :], w_all[l, 0]), mm(d_buf[tile(i), :], w_half[lax.rem(l, 2)])

    halve(last)
    h_buf[...], p_buf[...] = gelu_pair(*pre_pair(last, 0))
    y_buf[...], q_buf[...] = pre_pair(last, 1)

    def bwd_layer(k, c):
        l = last - k
        halve(jnp.maximum(l - 1, 0))

        def body(i, c):
            roll = lax.div(i + 2, nt)
            l_up = jnp.maximum(l - roll, 0)
            i_up = i + 2 - roll * nt
            y, gh = y_buf[...], q_buf[...]
            h, p = h_buf[...], p_buf[...]
            x = acts[l, tile(i), :].astype(F32)
            r = inv_norm(x)
            xr = x * r
            d_c = d_buf[tile(i), :]
            y_new, gh_new = pre_pair(l_up, i_up)
            gn = mm_nt(p, w_all[l, 0])
            d_up = mm_tn(nrm[l, tile(i), :], p)
            d_down = mm_tn(d_c, h)
            h_new, p_new = gelu_pair(y, gh)
            w = gn * (g_all[l][0:1, :] * root)
            d_in = d_c.astype(F32) + r * (w - xr * jnp.sum(w * xr, axis=-1, keepdims=True))
            d_gain = fold8(gn * xr)
            h_buf[...] = h_new
            p_buf[...] = p_new
            y_buf[...] = y_new
            q_buf[...] = gh_new
            grads[l, 0, 0:width, :] += d_up
            grads[l, 1, 0:width, :] += d_down
            grads[l, 0, width:width + 8, 0:width] += d_gain
            d_buf[tile(i), :] = d_in.astype(BF16)
            return c
        lax.fori_loop(0, nt, body, 0)
        loss_duties(k)
        duties(k)
        return c
    lax.fori_loop(0, n_layers, bwd_layer, 0)

    def tail(t, c):
        duties(t)
        return c
    lax.fori_loop(n_layers, n_layers + reach + 1, tail, 0)

    loss_ref[...] = l_send[len(flips)]
    up_ref[0] = grads[me, 0, 0:width, :] * 2.0
    down_ref[0] = grads[me, 1, 0:width, :].T
    gain_ref[0] = grads[me, 0, width:width + 8, 0:width] * root

    for cp in sent:
        cp.wait_send()

    def drain(l, c):
        @pl.when(lax.rem(l, 2) != core)
        def _():
            for half in (0, 1):
                for q in range(CHUNKS):
                    p_copy(l, half, q).wait_send()

        @pl.when((lax.rem(l, 2) == core) & (l != me))
        def _():
            for half in (0, 1):
                for q in range(CHUNKS):
                    c_copy(l, half, q, RIGHT).wait_send()
        return c
    lax.fori_loop(0, n_layers, drain, 0)


def solution(mesh):
    n = mesh.shape['stage']

    def device_step(inputs, targets, w_up, w_down, gains):
        n_micro, tokens, width = inputs.shape
        rows = n_micro * tokens // n
        norm_count = n_micro * tokens * width
        hid = w_up.shape[-1]
        layers = n
        steps = n.bit_length() - 1
        w_own = jnp.stack([w_up, jnp.swapaxes(w_down, 1, 2)], axis=1)
        g_own = jnp.broadcast_to(gains[:, None, :], (1, 8, width))
        vmem = pl.BlockSpec(memory_space=pltpu.VMEM)
        hbm = pl.BlockSpec(memory_space=pl.ANY)
        dma = pltpu.SemaphoreType.DMA
        pad = width + 8
        loss_part, d_up, d_down, d_gain = pl.pallas_call(
            functools.partial(kernel, n, norm_count),
            out_shape=(jax.ShapeDtypeStruct((8, width), F32), jax.ShapeDtypeStruct((1, width, hid), F32),
                       jax.ShapeDtypeStruct((1, hid, width), F32), jax.ShapeDtypeStruct((1, 8, width), F32)),
            in_specs=[hbm] * 4,
            out_specs=(vmem,) * 4,
            scratch_shapes=[
                pltpu.VMEM((layers, rows, width), BF16), pltpu.VMEM((layers, rows, width), BF16), pltpu.VMEM((rows, width), BF16),
                pltpu.VMEM((TILE, hid), F32), pltpu.VMEM((TILE, hid), F32), pltpu.VMEM((TILE, hid), BF16), pltpu.VMEM((TILE, hid), BF16),
                pltpu.VMEM((2, width, hid), BF16), pltpu.VMEM((layers, 2, width, hid), BF16), pltpu.VMEM((layers, 8, width), F32),
                pltpu.VMEM((layers, 2, pad, hid), F32), pltpu.VMEM((2, 2, pad, hid), F32), pltpu.VMEM((n // 2, 2, pad, hid), F32), pltpu.VMEM((2, pad, hid), F32),
                pltpu.VMEM((steps + 1, 8, width), F32), pltpu.VMEM((steps, 8, width), F32),
                dma((4,)), dma((3, layers, 2)), dma((layers, 2)), dma((3, layers)), dma((layers,)),
                dma((n // 2, 2, CHUNKS)), dma((n // 2, 2, CHUNKS)), dma((n // 2, 2, CHUNKS)), dma((n // 2, 2, CHUNKS)), dma((2, CHUNKS)),
                dma((steps,)), dma((steps,)), pltpu.SemaphoreType.REGULAR,
            ],
            compiler_params=pltpu.CompilerParams(collective_id=0, has_side_effects=True, vmem_limit_bytes=67043328),
        )(inputs.reshape(n_micro * tokens, width), targets.reshape(n_micro * tokens, width), w_own, g_own)
        return (jnp.sum(loss_part) / norm_count).reshape(1), d_up, d_down, jnp.sum(d_gain, axis=1)

    return jax.shard_map(device_step, mesh=mesh, in_specs=(P('dp', None, None), P('dp', None, None), P('stage', None, None), P('stage', None, None), P('stage', None)), out_specs=(P('dp'), P(('dp', 'stage'), None, None), P(('dp', 'stage'), None, None), P(('dp', 'stage'), None)), check_vma=False)
```

```python
import functools
import math
import jax
import jax.numpy as jnp
from jax import lax
from jax.experimental import pallas as pl
from jax.experimental.pallas import tpu as pltpu
from jax.sharding import PartitionSpec as P

NORM_EPS = 1e-6
GELU_C = math.sqrt(2.0 / math.pi)
K0 = 2.0 * GELU_C
K1 = 8.0 * GELU_C * 0.044715
TILE = 512
CHUNKS = 4
SUBS = 2
FINE = 3
RIGHT, LEFT, PARTNER = 0, 1, 2
F32 = jnp.float32
BF16 = jnp.bfloat16
MESH = pl.DeviceIdType.MESH


def mm(a, b):
    return lax.dot_general(a, b, (((1,), (0,)), ((), ())), preferred_element_type=F32)


def mm_nt(a, b):
    return lax.dot_general(a, b, (((1,), (1,)), ((), ())), preferred_element_type=F32)


def mm_tn(a, b):
    return lax.dot_general(a, b, (((0,), (0,)), ((), ())), preferred_element_type=F32)


def inv_norm(x):
    return lax.rsqrt(jnp.sum(x * x, axis=-1, keepdims=True) + NORM_EPS * x.shape[-1])


def fold8(z):
    return jnp.sum(z.reshape(-1, 8, z.shape[-1]), axis=0)


def gelu(y):
    t = jnp.tanh(y * (K1 * (y * y) + K0))
    return (y * (1.0 + t)).astype(BF16)


def gelu_pair(y, gh):
    q = y * y
    t = jnp.tanh(y * (K1 * q + K0))
    a = 1.0 + t
    hid = y * a
    slope = a + hid * ((1.0 - t) * ((3.0 * K1) * q + K0))
    return hid.astype(BF16), (gh * slope).astype(BF16)


def kernel(n, norm_count, x_hbm, y_hbm, up_hbm, down_hbm, gain_in, loss_ref, grad_out,
           acts, nrm, d_buf, y_buf, h_bufs, p_bufs, gn_bufs, w_half, w_all, g_all, grads, p_recv, c_recv, r_recv, l_send, l_recv,
           in_sem, w_send, w_rsem, g_send, g_rsem, p_ssem, p_rsem, c_ssem, c_rsem, r_rsem, l_ssem, l_rsem, credit):
    n_layers, _, width, hid_dim = w_all.shape
    rows = d_buf.shape[0]
    nz = n // 2
    root = math.sqrt(width)
    nt = rows // TILE
    last = n_layers - 1
    n_all = n_layers * nt
    step_rows = width // CHUNKS
    fine = [(q * step_rows, step_rows + (8 if q == CHUNKS - 1 else 0)) for q in range(CHUNKS)]
    coarse = [(0, width + 8)]

    me = lax.axis_index('stage')
    core, chip = lax.rem(me, 2), lax.div(me, 2)
    peers = (lax.rem(me + 2, n), lax.rem(me + n - 2, n), me + 1 - 2 * core)
    flips = [me + d * (1 - 2 * lax.rem(lax.div(me, d), 2)) for d in (1 << k for k in range(n.bit_length() - 1))]

    def push(src, dst, ssem, rsem, to):
        return pltpu.make_async_remote_copy(src_ref=src, dst_ref=dst, send_sem=ssem, recv_sem=rsem, device_id={'stage': to}, device_id_type=MESH)

    def tile(i):
        return pl.ds(pl.multiple_of(i * TILE, TILE), TILE)

    barrier = pltpu.get_barrier_semaphore()
    near = list(peers) + flips[2:]
    for to in near:
        pl.semaphore_signal(barrier, inc=1, device_id={'stage': to}, device_id_type=MESH)

    stage = nrm.at[0, pl.ds(0, hid_dim)]
    share = pl.ds(pl.multiple_of(me * rows, rows), rows)
    own = [pltpu.make_async_copy(down_hbm.at[0], stage, in_sem.at[0]), pltpu.make_async_copy(up_hbm.at[0], w_all.at[me, 0], in_sem.at[1])]
    data = [pltpu.make_async_copy(x_hbm.at[share], acts.at[0], in_sem.at[2]), pltpu.make_async_copy(y_hbm.at[share], d_buf, in_sem.at[3])]
    for cp in own + data:
        cp.start()
    g_all[me, 0:1, :] = gain_in[...]
    for cp in own:
        cp.wait()
    w_all[me, 1] = stage[...].T

    def zero(l, c):
        grads[l] = jnp.zeros(grads.shape[1:], F32)
        return c
    lax.fori_loop(0, n_layers, zero, 0)
    pl.semaphore_wait(barrier, len(near))

    sub_rows = width // SUBS

    def w_copy(layer, half, sub, way):
        ref = w_all.at[layer, half, pl.ds(sub * sub_rows, sub_rows)]
        return push(ref, ref, w_send.at[0], w_rsem.at[layer, half, sub], peers[way])

    def g_copy(layer, way):
        return push(g_all.at[layer], g_all.at[layer], g_send.at[0], g_rsem.at[layer], peers[way])

    pieces = [(half, sub) for half in (0, 1) for sub in range(SUBS)]
    for way in (RIGHT, LEFT, PARTNER):
        g_copy(me, way).start()
    for half, sub in pieces:
        for way in (RIGHT, LEFT, PARTNER):
            w_copy(me, half, sub, way).start()

    reach = nz // 2
    for j in range(1, reach + 1):
        ways = ((RIGHT, lax.rem(me + n - 2 * j, n)), (LEFT, lax.rem(me + 2 * j, n)))
        for way, layer in ways:
            if j < reach or way == RIGHT:
                g_copy(layer, way).wait_recv()
                if j < reach - (way == LEFT):
                    g_copy(layer, way).start()
                g_copy(layer, PARTNER).start()
        for half, sub in pieces:
            for way, layer in ways:
                far = reach if way == half else reach - 1
                if j <= far:
                    w_copy(layer, half, sub, way).wait_recv()
                    if j < far:
                        w_copy(layer, half, sub, way).start()
                    w_copy(layer, half, sub, PARTNER).start()

    def need(l):
        @pl.when(lax.rem(l, 2) != core)
        def _():
            g_copy(l, PARTNER).wait_recv()
            for half, sub in pieces:
                w_copy(l, half, sub, PARTNER).wait_recv()

    for cp in data:
        cp.wait()

    def norm_at(l, i):
        x = acts[l, tile(i), :].astype(F32)
        return (x * inv_norm(x) * (g_all[l][0:1, :] * (0.5 * root))).astype(BF16)

    need(0)
    for i in range(3):
        nrm[0, tile(i), :] = norm_at(0, i)
    h_bufs[0] = gelu(mm(nrm[0, tile(0), :], w_all[0, 0]))
    y_buf[...] = mm(nrm[0, tile(1), :], w_all[0, 0])

    def fwd_tile(l, i):
        idx = l * nt + i
        up = jnp.minimum(idx + 2, n_all - 1)
        nx = jnp.minimum(idx + 3, n_all - 1)
        l_up, i_up = lax.div(up, nt), lax.rem(up, nt)
        l_nx, i_nx = lax.div(nx, nt), lax.rem(nx, nt)
        y = y_buf[...]
        h = h_bufs[0]
        n_new = norm_at(l_nx, i_nx)
        out = acts[l, tile(i), :].astype(F32) + mm_nt(h, w_all[l, 1])
        y_new = mm(nrm[l_up, tile(i_up), :], w_all[l_up, 0])
        h_new = gelu(y)
        h_bufs[0] = h_new
        y_buf[...] = y_new
        nrm[l_nx, tile(i_nx), :] = n_new
        return out.astype(BF16)

    def fwd_layer(l, c):
        need(l + 1)

        def body(i, c):
            acts[l + 1, tile(i), :] = fwd_tile(l, i)
            return c
        return lax.fori_loop(0, nt, body, c)
    lax.fori_loop(0, last, fwd_layer, 0)

    def last_tile(i, acc):
        err = fwd_tile(last, i).astype(F32) - d_buf[tile(i), :].astype(F32)
        d_buf[tile(i), :] = (err * (2.0 / norm_count)).astype(BF16)
        return acc + fold8(err * err)
    l_send[0] = lax.fori_loop(0, nt, last_tile, jnp.zeros((8, width), F32))

    def part(ref, span):
        return ref.at[pl.ds(span[0], span[1])]

    def p_copy(l, half, q, span):
        s = lax.div(l, 2)
        return push(part(grads.at[l, half], span), part(p_recv.at[half], span), p_ssem.at[0], p_rsem.at[s, half, q], peers[PARTNER])

    def c_copy(l, half, q, span, way):
        s = lax.div(l, 2)
        return push(part(grads.at[l, half], span), part(c_recv.at[s, half], span), c_ssem.at[0], c_rsem.at[s, half, q], peers[way])

    def r_copy(l, half, q, span):
        return push(part(grads.at[l, half], span), part(r_recv.at[half], span), c_ssem.at[0], r_rsem.at[half, q], peers[LEFT])

    def add(l, half, span, src):
        a, m = span
        grads[l, half, pl.ds(a, m), :] += src[pl.ds(a, m), :]

    def to_root(l):
        return lax.rem(lax.div(l, 2) - chip + nz, nz)

    def give(l, spans):
        for half in (0, 1):
            for q, span in enumerate(spans):
                p_copy(l, half, q, span).start()

    def take(l, spans):
        for half in (0, 1):
            for q, span in enumerate(spans):
                p_copy(l, half, q, span).wait_recv()
                add(l, half, span, p_recv.at[half])

    def relay(l, half, way, pos, arc, spans):
        for q, span in enumerate(spans):
            if pos > 0:
                c_copy(l, half, q, span, way).wait_recv()
                add(l, half, span, c_recv.at[lax.div(l, 2), half])
            if way == LEFT and pos == arc - 1:
                r_copy(l, half, q, span).start()
            else:
                c_copy(l, half, q, span, way).start()

    def finish(l, spans):
        for half in (0, 1):
            for q, span in enumerate(spans):
                c_copy(l, half, q, span, RIGHT).wait_recv()
                add(l, half, span, c_recv.at[lax.div(l, 2), half])
                r_copy(l, half, q, span).wait_recv()
                add(l, half, span, r_recv.at[half])

    def sized(l, cond, fn):
        pl.when(cond & (l >= FINE))(lambda: fn(coarse))
        pl.when(cond & (l < FINE))(lambda: fn(fine))

    def duties(t):
        l0 = last - t

        @pl.when((l0 >= 0) & (lax.rem(l0 + n, 2) != core))
        def _():
            @pl.when(l0 <= last - 2)
            def _():
                pl.semaphore_wait(credit, 1)
            sized(l0, l0 >= 0, lambda spans: give(l0, spans))

        for s in range(reach + 1, 0, -1):
            l = l0 + s

            @pl.when((l >= 0) & (l <= last) & (lax.rem(l + n, 2) == core))
            def _(s=s, l=l):
                rd = to_root(l)
                if s == 1:
                    sized(l, l >= 0, lambda spans: take(l, spans))

                    @pl.when(l >= 2)
                    def _():
                        pl.semaphore_signal(credit, inc=1, device_id={'stage': peers[PARTNER]}, device_id_type=MESH)
                for half in (0, 1):
                    arc_r = reach - half
                    for way, arc, dist in ((RIGHT, arc_r, rd), (LEFT, nz - 1 - arc_r, nz - rd)):
                        pos = s - 1
                        if pos < arc:
                            sized(l, dist == arc - pos, functools.partial(relay, l, half, way, pos, arc))
                if s == reach + 1:
                    sized(l, rd == 0, functools.partial(finish, l))

    def l_copy(k):
        return push(l_send.at[k], l_recv.at[k], l_ssem.at[k], l_rsem.at[k], flips[k])

    def loss_duties(t):
        for k in range(len(flips)):
            @pl.when(t == 2 * k)
            def _(k=k):
                l_copy(k).start()

            @pl.when(t == 2 * k + 1)
            def _(k=k):
                l_copy(k).wait()
                l_send[k + 1] = l_send[k] + l_recv[k]

    def halve(l):
        w_half[lax.rem(l, 2)] = w_all[l, 1] * jnp.asarray(0.5, BF16)

    def inner(l, n_b, d_b):
        return gelu_pair(mm(n_b, w_all[l, 0]), mm(d_b, w_half[lax.rem(l, 2)]))

    def gradients(l, n_b, d_b, h, p):
        gn = jnp.concatenate([mm_nt(p[:TILE // 2], w_all[l, 0]), mm_nt(p[TILE // 2:], w_all[l, 0])], axis=0)
        d_up = mm_tn(n_b, p)
        d_down = mm_tn(d_b, h)
        grads[l, 0, 0:width, :] += d_up
        grads[l, 1, 0:width, :] += d_down
        return gn

    def norm_back(l, x_b, d_b, gn):
        x = x_b.astype(F32)
        r = inv_norm(x)
        xr = x * r
        w = gn * (g_all[l][0:1, :] * root)
        d_in = d_b.astype(F32) + r * (w - xr * jnp.sum(w * xr, axis=-1, keepdims=True))
        grads[l, 0, width:width + 8, 0:width] += fold8(gn * xr)
        return d_in.astype(BF16)

    def at(l, i):
        return nrm[l, tile(i), :], d_buf[tile(i), :]

    halve(last)
    h_bufs[0], p_bufs[0] = inner(last, *at(last, 0))
    gn_bufs[0] = gradients(last, *at(last, 0), h_bufs[0], p_bufs[0])
    h_bufs[1], p_bufs[1] = inner(last, *at(last, 1))

    def bwd_pair(l, j, ahead=(2, 2)):
        where = []
        for k in range(4):
            roll = lax.div(2 * j + k, nt)
            where.append((jnp.maximum(l - roll, 0), 2 * j + k - roll * nt))
        data = [at(*w) for w in where]
        xs = [acts[l, tile(2 * j + k), :] for k in range(2)]
        outs = []
        for k in range(2):
            outs.append(norm_back(l, xs[k], data[k][1], gn_bufs[k]))
            if ahead[k] > 1:
                h_bufs[k], p_bufs[k] = inner(where[k + 2][0], *data[k + 2])
            if ahead[k] > 0:
                gn_bufs[1 - k] = gradients(where[k + 1][0], *data[k + 1], h_bufs[1 - k], p_bufs[1 - k])
        for k in range(2):
            d_buf[tile(2 * j + k), :] = outs[k]

    def bwd_layer(k, c):
        l = last - k
        halve(l - 1)

        def body(j, c):
            bwd_pair(l, j)
            return c
        lax.fori_loop(0, nt // 2, body, 0)
        loss_duties(k)
        duties(k)
        return c
    lax.fori_loop(0, last, bwd_layer, 0)

    def first_body(j, c):
        bwd_pair(0, j)
        return c
    lax.fori_loop(0, nt // 2 - 1, first_body, 0)
    bwd_pair(0, nt // 2 - 1, ahead=(1, 0))

    def tail(t, c):
        duties(t)
        return c
    lax.fori_loop(last, n_layers + reach + 1, tail, 0)

    loss_ref[...] = l_send[len(flips)]
    result = pltpu.make_async_copy(grads.at[me], grad_out, in_sem.at[0])
    result.start()
    w_all_sent = w_all.at[pl.ds(0, n - 1)]
    g_all_sent = g_all.at[pl.ds(0, n - 1)]
    push(w_all_sent, w_all_sent, w_send.at[0], w_rsem.at[0, 0, 0], peers[0]).wait_send()
    push(g_all_sent, g_all_sent, g_send.at[0], g_rsem.at[0], peers[0]).wait_send()
    for count, sem in ((nz, p_ssem), (nz - 1, c_ssem)):
        ref = grads.at[pl.ds(0, count)]
        push(ref, ref, sem.at[0], r_rsem.at[0, 0], peers[0]).wait_send()
    result.wait()


def finish_kernel(norm_count, loss_ref, grad_ref, loss_out, up_out, down_out, gain_out):
    width = down_out.shape[-1]
    loss_out[0, 0] = jnp.sum(loss_ref[...]) / norm_count
    up_out[0] = grad_ref[0, 0:width, :] * 2.0
    down_out[0] = grad_ref[1, 0:width, :].T
    gain_out[...] = jnp.sum(grad_ref[0, width:width + 8, 0:width], axis=0, keepdims=True) * math.sqrt(width)


def solution(mesh):
    n = mesh.shape['stage']

    def device_step(inputs, targets, w_up, w_down, gains):
        n_micro, tokens, width = inputs.shape
        rows = n_micro * tokens // n
        norm_count = n_micro * tokens * width
        hid = w_up.shape[-1]
        layers = n
        steps = n.bit_length() - 1
        vmem = pl.BlockSpec(memory_space=pltpu.VMEM)
        smem = pl.BlockSpec(memory_space=pltpu.SMEM)
        hbm = pl.BlockSpec(memory_space=pl.ANY)
        dma = pltpu.SemaphoreType.DMA
        pad = width + 8
        loss_part, grad_own = pl.pallas_call(
            functools.partial(kernel, n, norm_count),
            out_shape=(jax.ShapeDtypeStruct((8, width), F32), jax.ShapeDtypeStruct((2, pad, hid), F32)),
            in_specs=[hbm] * 4 + [vmem],
            out_specs=(vmem, hbm),
            scratch_shapes=[
                pltpu.VMEM((layers, rows, width), BF16), pltpu.VMEM((layers, rows, width), BF16), pltpu.VMEM((rows, width), BF16),
                pltpu.VMEM((TILE, hid), F32), pltpu.VMEM((2, TILE, hid), BF16), pltpu.VMEM((2, TILE, hid), BF16),
                pltpu.VMEM((2, TILE, width), F32), pltpu.VMEM((2, width, hid), BF16), pltpu.VMEM((layers, 2, width, hid), BF16), pltpu.VMEM((layers, 8, width), F32),
                pltpu.VMEM((layers, 2, pad, hid), F32), pltpu.VMEM((2, pad, hid), F32), pltpu.VMEM((n // 2, 2, pad, hid), F32), pltpu.VMEM((2, pad, hid), F32),
                pltpu.VMEM((steps + 1, 8, width), F32), pltpu.VMEM((steps, 8, width), F32),
                dma((4,)), dma((1,)), dma((layers, 2, SUBS)), dma((1,)), dma((layers,)),
                dma((1,)), dma((n // 2, 2, CHUNKS)), dma((1,)), dma((n // 2, 2, CHUNKS)), dma((2, CHUNKS)),
                dma((steps,)), dma((steps,)), pltpu.SemaphoreType.REGULAR,
            ],
            compiler_params=pltpu.CompilerParams(collective_id=0, has_side_effects=True, vmem_limit_bytes=67043328),
        )(inputs.reshape(n_micro * tokens, width), targets.reshape(n_micro * tokens, width), w_up, w_down, gains)
        loss_value, d_up, d_down, d_gain = pl.pallas_call(
            functools.partial(finish_kernel, norm_count),
            out_shape=(jax.ShapeDtypeStruct((1, 1), F32), jax.ShapeDtypeStruct((1, width, hid), F32),
                       jax.ShapeDtypeStruct((1, hid, width), F32), jax.ShapeDtypeStruct((1, width), F32)),
            in_specs=[vmem] * 2,
            out_specs=(smem, vmem, vmem, vmem),
        )(loss_part, grad_own)
        return loss_value.reshape(1), d_up, d_down, d_gain

    return jax.shard_map(device_step, mesh=mesh, in_specs=(P('dp', None, None), P('dp', None, None), P('stage', None, None), P('stage', None, None), P('stage', None)), out_specs=(P('dp'), P(('dp', 'stage'), None, None), P(('dp', 'stage'), None, None), P(('dp', 'stage'), None)), check_vma=False)
```

```python
import functools
import math
import jax
import jax.numpy as jnp
from jax import lax
from jax.experimental import pallas as pl
from jax.experimental.pallas import tpu as pltpu
from jax.sharding import PartitionSpec as P

NORM_EPS = 1e-6
GELU_C = math.sqrt(2.0 / math.pi)
K0 = 2.0 * GELU_C
K1 = 8.0 * GELU_C * 0.044715
TILE = 512
CHUNKS = 4
SUBS = 2
FINE = 2
RIGHT, LEFT, PARTNER = 0, 1, 2
F32 = jnp.float32
BF16 = jnp.bfloat16
MESH = pl.DeviceIdType.MESH


def mm(a, b):
    return lax.dot_general(a, b, (((1,), (0,)), ((), ())), preferred_element_type=F32)


def mm_nt(a, b):
    return lax.dot_general(a, b, (((1,), (1,)), ((), ())), preferred_element_type=F32)


def mm_tn(a, b):
    return lax.dot_general(a, b, (((0,), (0,)), ((), ())), preferred_element_type=F32)


def inv_norm(x):
    return lax.rsqrt(jnp.sum(x * x, axis=-1, keepdims=True) + NORM_EPS * x.shape[-1])


def fold8(z):
    return jnp.sum(z.reshape(-1, 8, z.shape[-1]), axis=0)


def gelu(y):
    t = jnp.tanh(y * (K1 * (y * y) + K0))
    return (y * (1.0 + t)).astype(BF16)


def gelu_pair(y, gh):
    q = y * y
    t = jnp.tanh(y * (K1 * q + K0))
    a = 1.0 + t
    hid = y * a
    slope = a + hid * ((1.0 - t) * ((3.0 * K1) * q + K0))
    return hid.astype(BF16), (gh * slope).astype(BF16)


def kernel(n, norm_count, x_hbm, y_hbm, up_hbm, down_hbm, gain_in, loss_ref, grad_out,
           acts, nrm, d_buf, y_buf, h_bufs, p_bufs, gn_bufs, w_half, w_all, g_all, grads, p_recv, c_recv, r_recv, l_send, l_recv,
           in_sem, w_send, w_rsem, g_send, g_rsem, p_ssem, p_rsem, c_ssem, c_rsem, r_rsem, l_ssem, l_rsem, credit):
    n_layers, _, width, hid_dim = w_all.shape
    rows = d_buf.shape[0]
    nz = n // 2
    root = math.sqrt(width)
    nt = rows // TILE
    last = n_layers - 1
    n_all = n_layers * nt
    step_rows = width // CHUNKS
    fine = [(q * step_rows, step_rows + (8 if q == CHUNKS - 1 else 0)) for q in range(CHUNKS)]
    coarse = [(0, width + 8)]

    me = lax.axis_index('stage')
    core, chip = lax.rem(me, 2), lax.div(me, 2)
    peers = (lax.rem(me + 2, n), lax.rem(me + n - 2, n), me + 1 - 2 * core)
    flips = [me + d * (1 - 2 * lax.rem(lax.div(me, d), 2)) for d in (1 << k for k in range(n.bit_length() - 1))]

    def push(src, dst, ssem, rsem, to):
        return pltpu.make_async_remote_copy(src_ref=src, dst_ref=dst, send_sem=ssem, recv_sem=rsem, device_id={'stage': to}, device_id_type=MESH)

    def tile(i):
        return pl.ds(pl.multiple_of(i * TILE, TILE), TILE)

    barrier = pltpu.get_barrier_semaphore()
    near = list(peers) + flips[2:]
    for to in near:
        pl.semaphore_signal(barrier, inc=1, device_id={'stage': to}, device_id_type=MESH)

    stage = nrm.at[0, pl.ds(0, hid_dim)]
    share = pl.ds(pl.multiple_of(me * rows, rows), rows)
    own = [pltpu.make_async_copy(down_hbm.at[0], stage, in_sem.at[0]), pltpu.make_async_copy(up_hbm.at[0], w_all.at[me, 0], in_sem.at[1])]
    data = [pltpu.make_async_copy(x_hbm.at[share], acts.at[0], in_sem.at[2]), pltpu.make_async_copy(y_hbm.at[share], d_buf, in_sem.at[3])]
    for cp in own + data:
        cp.start()
    g_all[me, 0:1, :] = gain_in[...]
    for cp in own:
        cp.wait()
    w_all[me, 1] = stage[...].T

    def zero(l, c):
        grads[l] = jnp.zeros(grads.shape[1:], F32)
        return c
    lax.fori_loop(0, n_layers, zero, 0)
    pl.semaphore_wait(barrier, len(near))

    sub_rows = width // SUBS

    def w_copy(layer, half, sub, way):
        ref = w_all.at[layer, half, pl.ds(sub * sub_rows, sub_rows)]
        return push(ref, ref, w_send.at[0], w_rsem.at[layer, half, sub], peers[way])

    def g_copy(layer, way):
        return push(g_all.at[layer], g_all.at[layer], g_send.at[0], g_rsem.at[layer], peers[way])

    pieces = [(half, sub) for half in (0, 1) for sub in range(SUBS)]
    for way in (RIGHT, LEFT, PARTNER):
        g_copy(me, way).start()
    for half, sub in pieces:
        for way in (RIGHT, LEFT, PARTNER):
            w_copy(me, half, sub, way).start()

    reach = nz // 2
    for j in range(1, reach + 1):
        ways = ((RIGHT, lax.rem(me + n - 2 * j, n)), (LEFT, lax.rem(me + 2 * j, n)))
        for way, layer in ways:
            if j < reach or way == RIGHT:
                g_copy(layer, way).wait_recv()
                if j < reach - (way == LEFT):
                    g_copy(layer, way).start()
                g_copy(layer, PARTNER).start()
        for half, sub in pieces:
            for way, layer in ways:
                far = reach if way == half else reach - 1
                if j <= far:
                    w_copy(layer, half, sub, way).wait_recv()
                    if j < far:
                        w_copy(layer, half, sub, way).start()
                    w_copy(layer, half, sub, PARTNER).start()

    def need(l):
        @pl.when(lax.rem(l, 2) != core)
        def _():
            g_copy(l, PARTNER).wait_recv()
            for half, sub in pieces:
                w_copy(l, half, sub, PARTNER).wait_recv()

    for cp in data:
        cp.wait()

    def norm_at(l, i):
        x = acts[l, tile(i), :].astype(F32)
        return (x * inv_norm(x) * (g_all[l][0:1, :] * (0.5 * root))).astype(BF16)

    need(0)
    for i in range(3):
        nrm[0, tile(i), :] = norm_at(0, i)
    h_bufs[0] = gelu(mm(nrm[0, tile(0), :], w_all[0, 0]))
    y_buf[...] = mm(nrm[0, tile(1), :], w_all[0, 0])

    def fwd_tile(l, i):
        idx = l * nt + i
        up = jnp.minimum(idx + 2, n_all - 1)
        nx = jnp.minimum(idx + 3, n_all - 1)
        l_up, i_up = lax.div(up, nt), lax.rem(up, nt)
        l_nx, i_nx = lax.div(nx, nt), lax.rem(nx, nt)
        y = y_buf[...]
        h = h_bufs[0]
        n_new = norm_at(l_nx, i_nx)
        out = acts[l, tile(i), :].astype(F32) + mm_nt(h, w_all[l, 1])
        y_new = mm(nrm[l_up, tile(i_up), :], w_all[l_up, 0])
        h_new = gelu(y)
        h_bufs[0] = h_new
        y_buf[...] = y_new
        nrm[l_nx, tile(i_nx), :] = n_new
        return out.astype(BF16)

    def fwd_layer(l, c):
        need(l + 1)

        def body(i, c):
            acts[l + 1, tile(i), :] = fwd_tile(l, i)
            return c
        return lax.fori_loop(0, nt, body, c)
    lax.fori_loop(0, last, fwd_layer, 0)

    def last_tile(i, acc):
        err = fwd_tile(last, i).astype(F32) - d_buf[tile(i), :].astype(F32)
        d_buf[tile(i), :] = (err * (2.0 / norm_count)).astype(BF16)
        return acc + fold8(err * err)
    l_send[0] = lax.fori_loop(0, nt, last_tile, jnp.zeros((8, width), F32))

    def part(ref, span):
        return ref.at[pl.ds(span[0], span[1])]

    def p_copy(l, half, q, span):
        s = lax.div(l, 2)
        return push(part(grads.at[l, half], span), part(p_recv.at[half], span), p_ssem.at[0], p_rsem.at[s, half, q], peers[PARTNER])

    def c_copy(l, half, q, span, way):
        s = lax.div(l, 2)
        return push(part(grads.at[l, half], span), part(c_recv.at[s, half], span), c_ssem.at[0], c_rsem.at[s, half, q], peers[way])

    def r_copy(l, half, q, span):
        return push(part(grads.at[l, half], span), part(r_recv.at[half], span), c_ssem.at[0], r_rsem.at[half, q], peers[LEFT])

    def add(l, half, span, src):
        a, m = span
        grads[l, half, pl.ds(a, m), :] += src[pl.ds(a, m), :]

    def to_root(l):
        return lax.rem(lax.div(l, 2) - chip + nz, nz)

    def give(l, half, spans):
        for q, span in enumerate(spans):
            p_copy(l, half, q, span).start()

    def take(l, half, spans):
        for q, span in enumerate(spans):
            p_copy(l, half, q, span).wait_recv()
            add(l, half, span, p_recv.at[half])

    def relay(l, half, way, pos, arc, spans):
        for q, span in enumerate(spans):
            if pos > 0:
                c_copy(l, half, q, span, way).wait_recv()
                add(l, half, span, c_recv.at[lax.div(l, 2), half])
            if way == LEFT and pos == arc - 1:
                r_copy(l, half, q, span).start()
            else:
                c_copy(l, half, q, span, way).start()

    def finish(l, half, spans):
        for q, span in enumerate(spans):
            c_copy(l, half, q, span, RIGHT).wait_recv()
            add(l, half, span, c_recv.at[lax.div(l, 2), half])
            r_copy(l, half, q, span).wait_recv()
            add(l, half, span, r_recv.at[half])

    def sized(l, fn):
        pl.when(l >= FINE)(lambda: fn(coarse))
        pl.when(l < FINE)(lambda: fn(fine))

    far_r = reach + 1
    far_l = nz - 1 - far_r
    plan = {s: [(RIGHT, s - 1, far_r)] for s in range(1, far_r + 1)}
    plan[1] = plan[1] + [(LEFT, 0, far_l)]
    plan[far_r] = plan[far_r] + [(LEFT, 1, far_l)]

    def duties(t, halves):
        l0 = last - t

        @pl.when((l0 >= 0) & (l0 <= last) & (lax.rem(l0 + n, 2) != core))
        def _():
            for half in halves:
                @pl.when(l0 <= last - 2)
                def _(half=half):
                    pl.semaphore_wait(credit.at[half], 1)
                sized(l0, functools.partial(give, l0, half))

        for s in range(far_r + 1, 0, -1):
            l = l0 + s

            @pl.when((l >= 0) & (l <= last) & (lax.rem(l + n, 2) == core))
            def _(s=s, l=l):
                rd = to_root(l)
                for half in halves:
                    if s == 1:
                        sized(l, functools.partial(take, l, half))

                        @pl.when(l >= 2)
                        def _(half=half):
                            pl.semaphore_signal(credit.at[half], inc=1, device_id={'stage': peers[PARTNER]}, device_id_type=MESH)
                    pos = s - 1
                    arc_r = reach - half
                    for way, arc, dist in ((RIGHT, arc_r, rd), (LEFT, nz - 1 - arc_r, nz - rd)):
                        if pos < arc:
                            pl.when((l < FINE) & (dist == arc - pos))(functools.partial(relay, l, half, way, pos, arc, fine))
                    for way, pos, arc in plan.get(s, []):
                        dist = rd if way == RIGHT else nz - rd
                        pl.when((l >= FINE) & (dist == arc - pos))(functools.partial(relay, l, half, way, pos, arc, coarse))
                    if s == reach + 1:
                        pl.when((l < FINE) & (rd == 0))(functools.partial(finish, l, half, fine))
                    if s == far_r + 1:
                        pl.when((l >= FINE) & (rd == 0))(functools.partial(finish, l, half, coarse))

    def l_copy(k):
        return push(l_send.at[k], l_recv.at[k], l_ssem.at[k], l_rsem.at[k], flips[k])

    def loss_duties(t):
        for k in range(len(flips)):
            @pl.when(t == 2 * k)
            def _(k=k):
                l_copy(k).start()

            @pl.when(t == 2 * k + 1)
            def _(k=k):
                l_copy(k).wait()
                l_send[k + 1] = l_send[k] + l_recv[k]

    def halve(l):
        w_half[lax.rem(l, 2)] = w_all[l, 1] * jnp.asarray(0.5, BF16)

    def inner(l, n_b, d_b):
        return gelu_pair(mm(n_b, w_all[l, 0]), mm(d_b, w_half[lax.rem(l, 2)]))

    def gradients(l, n_b, d_b, h, p):
        gn = jnp.concatenate([mm_nt(p[:TILE // 2], w_all[l, 0]), mm_nt(p[TILE // 2:], w_all[l, 0])], axis=0)
        d_up = mm_tn(n_b, p)
        d_down = mm_tn(d_b, h)
        grads[l, 0, 0:width, :] += d_up
        grads[l, 1, 0:width, :] += d_down
        return gn

    def norm_back(l, x_b, d_b, gn):
        x = x_b.astype(F32)
        r = inv_norm(x)
        xr = x * r
        w = gn * (g_all[l][0:1, :] * root)
        d_in = d_b.astype(F32) + r * (w - xr * jnp.sum(w * xr, axis=-1, keepdims=True))
        grads[l, 0, width:width + 8, 0:width] += fold8(gn * xr)
        return d_in.astype(BF16)

    def at(l, i):
        return nrm[l, tile(i), :], d_buf[tile(i), :]

    halve(last)
    h_bufs[0], p_bufs[0] = inner(last, *at(last, 0))
    gn_bufs[0] = gradients(last, *at(last, 0), h_bufs[0], p_bufs[0])
    h_bufs[1], p_bufs[1] = inner(last, *at(last, 1))

    def bwd_pair(l, j, ahead=(2, 2)):
        where = []
        for k in range(4):
            roll = lax.div(2 * j + k, nt)
            where.append((jnp.maximum(l - roll, 0), 2 * j + k - roll * nt))
        data = [at(*w) for w in where]
        xs = [acts[l, tile(2 * j + k), :] for k in range(2)]
        outs = []
        for k in range(2):
            outs.append(norm_back(l, xs[k], data[k][1], gn_bufs[k]))
            if ahead[k] > 1:
                h_bufs[k], p_bufs[k] = inner(where[k + 2][0], *data[k + 2])
            if ahead[k] > 0:
                gn_bufs[1 - k] = gradients(where[k + 1][0], *data[k + 1], h_bufs[1 - k], p_bufs[1 - k])
        for k in range(2):
            d_buf[tile(2 * j + k), :] = outs[k]

    def bwd_layer(k, c):
        l = last - k
        halve(l - 1)

        def body(j, c):
            bwd_pair(l, j)
            return c
        lax.fori_loop(0, nt // 4, body, 0)
        duties(k - 1, (1,))
        lax.fori_loop(nt // 4, nt // 2, body, 0)
        loss_duties(k)
        duties(k, (0,))
        return c
    lax.fori_loop(0, last, bwd_layer, 0)

    def first_body(j, c):
        bwd_pair(0, j)
        return c
    lax.fori_loop(0, nt // 4, first_body, 0)
    duties(last - 1, (1,))
    lax.fori_loop(nt // 4, nt // 2 - 1, first_body, 0)
    bwd_pair(0, nt // 2 - 1, ahead=(1, 0))

    def tail(t, c):
        duties(t, (0, 1))
        return c
    lax.fori_loop(last, n_layers + reach + 1, tail, 0)

    loss_ref[...] = l_send[len(flips)]
    result = pltpu.make_async_copy(grads.at[me], grad_out, in_sem.at[0])
    result.start()
    w_all_sent = w_all.at[pl.ds(0, n - 1)]
    g_all_sent = g_all.at[pl.ds(0, n - 1)]
    push(w_all_sent, w_all_sent, w_send.at[0], w_rsem.at[0, 0, 0], peers[0]).wait_send()
    push(g_all_sent, g_all_sent, g_send.at[0], g_rsem.at[0], peers[0]).wait_send()
    for count, sem in ((nz, p_ssem), (nz - 1, c_ssem)):
        ref = grads.at[pl.ds(0, count)]
        push(ref, ref, sem.at[0], r_rsem.at[0, 0], peers[0]).wait_send()
    result.wait()


def finish_kernel(norm_count, loss_ref, grad_ref, loss_out, up_out, down_out, gain_out):
    width = down_out.shape[-1]
    loss_out[0, 0] = jnp.sum(loss_ref[...]) / norm_count
    up_out[0] = grad_ref[0, 0:width, :] * 2.0
    down_out[0] = grad_ref[1, 0:width, :].T
    gain_out[...] = jnp.sum(grad_ref[0, width:width + 8, 0:width], axis=0, keepdims=True) * math.sqrt(width)


def solution(mesh):
    n = mesh.shape['stage']

    def device_step(inputs, targets, w_up, w_down, gains):
        n_micro, tokens, width = inputs.shape
        rows = n_micro * tokens // n
        norm_count = n_micro * tokens * width
        hid = w_up.shape[-1]
        layers = n
        steps = n.bit_length() - 1
        vmem = pl.BlockSpec(memory_space=pltpu.VMEM)
        smem = pl.BlockSpec(memory_space=pltpu.SMEM)
        hbm = pl.BlockSpec(memory_space=pl.ANY)
        dma = pltpu.SemaphoreType.DMA
        pad = width + 8
        loss_part, grad_own = pl.pallas_call(
            functools.partial(kernel, n, norm_count),
            out_shape=(jax.ShapeDtypeStruct((8, width), F32), jax.ShapeDtypeStruct((2, pad, hid), F32)),
            in_specs=[hbm] * 4 + [vmem],
            out_specs=(vmem, hbm),
            scratch_shapes=[
                pltpu.VMEM((layers, rows, width), BF16), pltpu.VMEM((layers, rows, width), BF16), pltpu.VMEM((rows, width), BF16),
                pltpu.VMEM((TILE, hid), F32), pltpu.VMEM((2, TILE, hid), BF16), pltpu.VMEM((2, TILE, hid), BF16),
                pltpu.VMEM((2, TILE, width), F32), pltpu.VMEM((2, width, hid), BF16), pltpu.VMEM((layers, 2, width, hid), BF16), pltpu.VMEM((layers, 8, width), F32),
                pltpu.VMEM((layers, 2, pad, hid), F32), pltpu.VMEM((2, pad, hid), F32), pltpu.VMEM((n // 2, 2, pad, hid), F32), pltpu.VMEM((2, pad, hid), F32),
                pltpu.VMEM((steps + 1, 8, width), F32), pltpu.VMEM((steps, 8, width), F32),
                dma((4,)), dma((1,)), dma((layers, 2, SUBS)), dma((1,)), dma((layers,)),
                dma((1,)), dma((n // 2, 2, CHUNKS)), dma((1,)), dma((n // 2, 2, CHUNKS)), dma((2, CHUNKS)),
                dma((steps,)), dma((steps,)), pltpu.SemaphoreType.REGULAR((2,)),
            ],
            compiler_params=pltpu.CompilerParams(collective_id=0, has_side_effects=True, vmem_limit_bytes=67043328),
        )(inputs.reshape(n_micro * tokens, width), targets.reshape(n_micro * tokens, width), w_up, w_down, gains)
        loss_value, d_up, d_down, d_gain = pl.pallas_call(
            functools.partial(finish_kernel, norm_count),
            out_shape=(jax.ShapeDtypeStruct((1, 1), F32), jax.ShapeDtypeStruct((1, width, hid), F32),
                       jax.ShapeDtypeStruct((1, hid, width), F32), jax.ShapeDtypeStruct((1, width), F32)),
            in_specs=[vmem] * 2,
            out_specs=(smem, vmem, vmem, vmem),
        )(loss_part, grad_own)
        return loss_value.reshape(1), d_up, d_down, d_gain

    return jax.shard_map(device_step, mesh=mesh, in_specs=(P('dp', None, None), P('dp', None, None), P('stage', None, None), P('stage', None, None), P('stage', None)), out_specs=(P('dp'), P(('dp', 'stage'), None, None), P(('dp', 'stage'), None, None), P(('dp', 'stage'), None)), check_vma=False)
```
